32 devices in a mesh: subj: 8 (over y, x, core), feat: 4 (over z).
Axes of the slice: x: 2, y: 2, z: 4, core: 2. Of those that a mesh axis runs over, the one named last changes fastest.
Arguments:
- records: float32 [8192, 16384], P('subj', 'feat'), may hold values from -6 to 6
- feature_factor: float32 [16384, 64], P('feat'), may hold values from -0.046875 to 0.046875
- mixing: float32 [64, 64], replicated, may hold values from -0.75 to 0.75
- weights: float32 [32, 64], P('subj'), may hold values from 0.3 to 3
- visits: int32 [32], P('subj'), may hold values from 128 to 640, as said below
Outputs:
- new_factor: float32 [16384, 64], P('feat')
- new_mixing: float32 [64, 64], replicated
- new_weights: float32 [32, 64], P('subj')
The draws below stay inside these ranges and needn't reach their ends.
Inputs may be any that keep to these rules, and one draw needn't show every extreme that they name: The visits of subjects b * 4 to b * 4 + 3 sum to 1024 for every b.
All inputs are finite; a program needn't handle non-finite values.
Results may differ from the reference program's by a relative error of at most 0.0005.
Values sent between devices are 32-bit elements; how exact they have to be, the bound alone decides.
A program may use at most 64 MiB of HBM per device.

```python
import math
import jax
import jax.numpy as jnp
from jax import lax

J = 16384
R = 64
SUB_DEV = 4
ROW_DEV = 1024
ITERS = 3
NS_ITERS = 8
SUBJECTS = 32
ROWS = 8192


def draw_visits(key, part):
    blocks = SUBJECTS // SUB_DEV
    spare = ROW_DEV - 2 * R * SUB_DEV
    cuts = jax.random.randint(jax.random.fold_in(key, 11), (blocks, SUB_DEV - 1), 0, spare + 1)
    cuts = jnp.sort(cuts, axis=1)
    edges = jnp.concatenate([jnp.zeros((blocks, 1), jnp.int32), cuts.astype(jnp.int32), jnp.full((blocks, 1), spare, jnp.int32)], axis=1)
    extra = edges[:, 1:] - edges[:, :-1]
    hot_block = jax.random.randint(jax.random.fold_in(key, 12), (), 0, blocks)
    hot_slot = jax.random.randint(jax.random.fold_in(key, 13), (), 0, SUB_DEV)
    block_ids = jnp.arange(blocks, dtype=jnp.int32)[:, None]
    slot_ids = jnp.arange(SUB_DEV, dtype=jnp.int32)[None, :]
    loaded = jnp.where(slot_ids == hot_slot, spare, 0).astype(jnp.int32)
    extra = jnp.where(block_ids == hot_block, loaded, extra)
    return (extra + 2 * R).reshape(-1).astype(jnp.int32)


def shard_levels(rng, dims, shards, low, top_value):
    loudness = 1.0
    for dim, parts in shards:
        steps = jax.random.uniform(jax.random.fold_in(jax.random.fold_in(rng, 6), dim), (parts,), jnp.float32, low / len(shards), top_value / len(shards))
        loudness = loudness * jnp.repeat(jnp.exp(steps), dims[dim] // parts).reshape((-1,) + (1,) * (len(dims) - 1 - dim))
    return loudness


def gaussian(rng, dims, deviation, limit, cuts=(), held_as=jnp.bfloat16):
    array = deviation * jax.random.normal(rng, dims, jnp.float32)
    if cuts:
        array = array * shard_levels(rng, dims, cuts, -0.22, 0.18)
    return jnp.clip(array, -limit, limit).astype(held_as)


def setup_inputs(seed: int = 0) -> dict:
    key_of = jax.random.split(jax.random.key(seed), 6)
    return {
        "records": gaussian(key_of[0], (ROWS, J), 1.0, 6.0, ((0, 8), (1, 4)), jnp.float32),
        "feature_factor": gaussian(key_of[1], (J, R), J ** -0.5, 0.046875, ((0, 4),), jnp.float32),
        "mixing": gaussian(key_of[2], (R, R), R ** -0.5, 0.75, (), jnp.float32),
        "weights": jnp.clip(jnp.exp(math.log(3.0) - 2.3025851 * jax.random.uniform(key_of[3], (SUBJECTS, R), jnp.float32) ** shard_levels(key_of[3], (SUBJECTS, R), ((0, 8),), -0.2, 0.2)), 0.3, 3.0),
        "visits": draw_visits(jax.random.fold_in(key_of[5], 71), 0),
    }


HIGH = lax.Precision.HIGHEST

def slot_table(counts, rows):
    ends = jnp.cumsum(counts)
    starts = ends - counts
    position = lax.broadcasted_iota(jnp.int32, (rows, counts.shape[0]), 0)
    return ((position >= starts[None, :]) & (position < ends[None, :])).astype(jnp.float32)

def inverse_root(gram):
    size = gram.shape[-1]
    scale = jnp.trace(gram, axis1=1, axis2=2) + 1e-06
    ident = jnp.broadcast_to(jnp.eye(size, dtype=jnp.float32), gram.shape)
    upper = gram / scale[:, None, None]
    lower = ident
    for step in range(NS_ITERS):
        middle = 1.5 * ident - 0.5 * jnp.einsum('kab,kbc->kac', lower, upper, precision=HIGH)
        upper, lower = (jnp.einsum('kab,kbc->kac', upper, middle, precision=HIGH), jnp.einsum('kab,kbc->kac', middle, lower, precision=HIGH))
    return lower / jnp.sqrt(scale)[:, None, None]

def solve_gram(gram, rhs):
    factor = jnp.linalg.cholesky(gram)
    return jax.scipy.linalg.cho_solve((factor, True), rhs.T).T

def reference(records, feature_factor, mixing, weights, visits):
    blocks = SUBJECTS // SUB_DEV
    slots = jax.vmap(lambda c: slot_table(c, ROW_DEV))(visits.reshape(blocks, SUB_DEV))
    factor, mix, wts = (feature_factor, mixing, weights)
    for outer in range(ITERS):
        projected = jnp.dot(records.astype(jnp.float32), factor.astype(jnp.float32), precision=HIGH, preferred_element_type=jnp.float32)
        vgram = jnp.dot(factor.T.astype(jnp.float32), factor.astype(jnp.float32), precision=HIGH, preferred_element_type=jnp.float32)
        proj = projected.reshape(blocks, ROW_DEV, R)
        wrow = jnp.einsum('bns,bsr->bnr', slots, wts.reshape(blocks, SUB_DEV, R), precision=HIGH)
        mixed = jnp.einsum('bnr,qr->bnq', proj * wrow, mix, precision=HIGH)
        spread = slots[:, :, :, None] * mixed[:, :, None, :]
        gram = jnp.einsum('bnsr,bnq->bsrq', spread, mixed, precision=HIGH).reshape(SUBJECTS, R, R)
        cross = jnp.einsum('bnsr,bnq->bsrq', spread, proj, precision=HIGH).reshape(SUBJECTS, R, R)
        root = inverse_root(gram)
        core = jnp.einsum('krq,kqp->krp', root, cross, precision=HIGH)
        msum = jnp.einsum('krq,kq->rq', core, wts, precision=HIGH)
        wgram = jnp.dot(wts.T.astype(jnp.float32), wts.astype(jnp.float32), precision=HIGH, preferred_element_type=jnp.float32)
        mix_new = solve_gram(vgram * wgram, msum)
        hgram = jnp.dot(mix_new.T.astype(jnp.float32), mix_new.astype(jnp.float32), precision=HIGH, preferred_element_type=jnp.float32)
        wtarget = jnp.einsum('rq,krq->kq', mix_new, core, precision=HIGH)
        wts_new = solve_gram(hgram * vgram, wtarget)
        rotated = jnp.einsum('bnr,bsrq->bnsq', mixed, root.reshape(blocks, SUB_DEV, R, R), precision=HIGH)
        ortho = lax.optimization_barrier(jnp.sum(rotated * slots[:, :, :, None], axis=2))
        wrow_new = jnp.einsum('bns,bsr->bnr', slots, wts_new.reshape(blocks, SUB_DEV, R), precision=HIGH)
        basis = jnp.einsum('bnq,qp->bnp', ortho, mix_new, precision=HIGH) * wrow_new
        total = jnp.einsum('nj,nr->jr', records, basis.reshape(ROWS, R), precision=HIGH)
        wgram_new = jnp.dot(wts_new.T.astype(jnp.float32), wts_new.astype(jnp.float32), precision=HIGH, preferred_element_type=jnp.float32)
        factor = solve_gram(hgram * wgram_new, total)
        mix, wts = (mix_new, wts_new)
    return (factor, mix, wts)
```

```python
import functools

import jax
import jax.numpy as jnp
from jax import lax
from jax.experimental import pallas as pl
from jax.experimental.pallas import tpu as pltpu
from jax.sharding import PartitionSpec as P

ITERS = 3
NS_ITERS = 8
SUBLANES = 8
HIGH = lax.Precision.HIGHEST
BIG = lax.Precision.HIGH
MESH = pl.DeviceIdType.MESH
F32 = jnp.float32


def slot_rows(counts, rows, padded):
    ends = jnp.cumsum(counts)
    starts = ends - counts
    position = lax.broadcasted_iota(jnp.int32, (counts.shape[0], rows), 1)
    mask = ((position >= starts[:, None]) & (position < ends[:, None])).astype(F32)
    return jnp.pad(mask, ((0, padded - counts.shape[0]), (0, 0)))


def dot(a, b, dims=((1,), (0,))):
    return lax.dot_general(a, b, (dims, ((), ())), precision=HIGH, preferred_element_type=F32)


TN = ((0,), (0,))
NT = ((1,), (1,))


def spd_inverse(a):
    size = a.shape[0]
    row_id = lax.broadcasted_iota(jnp.int32, a.shape, 0)
    col_id = lax.broadcasted_iota(jnp.int32, a.shape, 1)
    for k in range(size):
        col = a[:, k : k + 1]
        scale = 1.0 / a[k : k + 1, k : k + 1]
        a = jnp.where(col_id == k, (row_id == k).astype(F32), a)
        row = a[k : k + 1, :] * scale
        a = jnp.where(row_id == k, row, a - col * row)
    return a


def peer_of(axis, n, k):
    return lax.rem(lax.axis_index(axis) + k, n)


def greet(groups):
    barrier = pltpu.get_barrier_semaphore()
    count = 0
    for axis, n in groups:
        for k in range(1, n):
            pl.semaphore_signal(barrier, inc=1, device_id={axis: peer_of(axis, n, k)}, device_id_type=MESH)
            count += 1
    if count:
        pl.semaphore_wait(barrier, count)


def send_all(src_of, dst_of, sems, axis, n):
    copies = []
    for k in range(1, n):
        peer = peer_of(axis, n, k)
        copy = pltpu.make_async_remote_copy(
            src_ref=src_of(peer),
            dst_ref=dst_of(k),
            send_sem=sems.at[0, k - 1],
            recv_sem=sems.at[1, k - 1],
            device_id={axis: peer},
            device_id_type=MESH,
        )
        copy.start()
        copies.append(copy)
    return copies


def wait_recv(copies):
    for copy in copies:
        copy.wait_recv()


def wait_send(copies):
    for copy in copies:
        copy.wait_send()


def chunk(index, size):
    return pl.ds(pl.multiple_of(index * size, SUBLANES), size)


def scatter_start(x_ref, part, sems, axis, n):
    size = x_ref.shape[0] // n
    return send_all(lambda peer: x_ref.at[chunk(peer, size)], lambda k: part.at[k - 1], sems, axis, n)


def scatter_finish(x_ref, copies, part, mine, full, sems, axis, n):
    size = x_ref.shape[0] // n
    me = lax.axis_index(axis)
    wait_recv(copies)
    acc = x_ref[chunk(me, size), :]
    for k in range(1, n):
        acc = acc + part[k - 1]
    mine[...] = acc
    gather = send_all(lambda peer: mine, lambda k: full.at[chunk(me, size)], sems, axis, n)
    full[chunk(me, size), :] = acc
    wait_recv(gather)
    wait_send(copies)
    wait_send(gather)


def exchange_start(src, slots, sems, axis, n):
    return send_all(lambda peer: src, lambda k: slots.at[lax.axis_index(axis)], sems, axis, n)


def exchange_finish(src, copies, slots, axis, n):
    wait_recv(copies)
    slots[lax.axis_index(axis)] = src[...]
    total = slots[0]
    for k in range(1, n):
        total = total + slots[k]
    wait_send(copies)
    return total


def mix_kernel(subjects, nf, ns, ring, proj_ref, vg_ref, wg_ref, wts_ref, mix_ref, mask_ref,
               mix_out, hg_out, wts_out, wgl_out, basis_out, vg_out,
               part, mine, full, vslots, mslots, msend, spread, p_sem, g_sem, v_sem, m_sem):
    size = mix_ref.shape[0]
    greet((("feat", nf), ("subj", ns)))
    vcopies = exchange_start(vg_ref, vslots, v_sem, "feat", nf)
    if ring:
        copies = scatter_start(proj_ref, part, p_sem, "feat", nf)
    vgram = exchange_finish(vg_ref, vcopies, vslots, "feat", nf)
    vg_out[...] = vgram
    mix_inv = spd_inverse(vgram * wg_ref[...])
    if ring:
        scatter_finish(proj_ref, copies, part, mine, full, g_sem, "feat", nf)
        proj = full[...]
    else:
        proj = proj_ref[...]
    mask = mask_ref[...]
    wts = wts_ref[...]
    mixed = dot(mix_ref[...], proj * dot(wts, mask, TN))
    for s in range(subjects):
        spread[s * size : (s + 1) * size, :] = mixed * mask[s : s + 1, :]
    gram = dot(spread[...], mixed, NT)
    cross = dot(spread[...], proj, NT)
    eye = (lax.broadcasted_iota(jnp.int32, (size, size), 0)
           == lax.broadcasted_iota(jnp.int32, (size, size), 1)).astype(F32)
    uppers, lowers, scales = [], [], []
    for s in range(subjects):
        g = gram[s * size : (s + 1) * size, :]
        scale = jnp.sum(jnp.sum(g * eye, axis=1, keepdims=True), axis=0, keepdims=True) + 1e-06
        scales.append(scale)
        uppers.append(g / scale)
        lowers.append(eye)
    for step in range(NS_ITERS):
        for s in range(subjects):
            low_up = uppers[s] if step == 0 else dot(lowers[s], uppers[s])
            middle = 1.5 * eye - 0.5 * low_up
            lowers[s] = middle if step == 0 else dot(middle, lowers[s])
            if step < NS_ITERS - 1:
                uppers[s] = dot(uppers[s], middle)
    roots = [lowers[s] / jnp.sqrt(scales[s]) for s in range(subjects)]
    cores = [dot(roots[s], cross[s * size : (s + 1) * size, :]) for s in range(subjects)]
    msum = cores[0] * wts[0:1, :]
    for s in range(1, subjects):
        msum = msum + cores[s] * wts[s : s + 1, :]
    msend[...] = msum
    mcopies = exchange_start(msend, mslots, m_sem, "subj", ns)
    msum = exchange_finish(msend, mcopies, mslots, "subj", ns)
    mix_new = dot(msum, mix_inv)
    mix_out[...] = mix_new
    hgram = dot(mix_new, mix_new, TN)
    hg_out[...] = hgram
    turned = jnp.concatenate([dot(roots[s], mix_new) for s in range(subjects)], axis=0)
    ortho = dot(turned, spread[...], TN)
    target_row = lax.broadcasted_iota(jnp.int32, wts.shape, 0)
    target = jnp.zeros_like(wts)
    for s in range(subjects):
        target = jnp.where(target_row == s, jnp.sum(cores[s] * mix_new, axis=0, keepdims=True), target)
    wts_new = dot(target, spd_inverse(hgram * vgram))
    wts_out[...] = wts_new
    wgl_out[...] = dot(wts_new, wts_new, TN)
    basis_out[...] = ortho * dot(wts_new, mask, TN)


def factor_kernel(ns, ring, total_ref, wgl_ref, hg_ref, fac_out, wg_out, vgl_out,
                  part, mine, full, wslots, p_sem, g_sem, w_sem):
    greet((("subj", ns),))
    wcopies = exchange_start(wgl_ref, wslots, w_sem, "subj", ns)
    if ring:
        copies = scatter_start(total_ref, part, p_sem, "subj", ns)
    wgram = exchange_finish(wgl_ref, wcopies, wslots, "subj", ns)
    wg_out[...] = wgram
    inverse = spd_inverse(hg_ref[...] * wgram)
    if ring:
        scatter_finish(total_ref, copies, part, mine, full, g_sem, "subj", ns)
        total = full
    else:
        total = total_ref
    gram = jnp.zeros_like(wgram)
    width = total.shape[1]
    piece = min(width, 1024)
    for start in range(0, width, piece):
        value = dot(inverse, total[:, start : start + piece])
        fac_out[:, start : start + piece] = value
        gram = gram + dot(value, value, NT)
    vgl_out[...] = gram


def sems(n):
    return pltpu.SemaphoreType.DMA((2, max(n - 1, 1)))


def ring_scratch(shape, n, ring):
    rows = shape[0] // n if ring else SUBLANES
    cols = shape[1] if ring else 128
    return [
        pltpu.VMEM((max(n - 1, 1), rows, cols), F32),
        pltpu.VMEM((rows, cols), F32),
        pltpu.VMEM(shape if ring else (SUBLANES, 128), F32),
    ]


def mix_call(subjects, nf, ns, proj, vgl, wgram, wts, mix, mask):
    size = mix.shape[0]
    square = jax.ShapeDtypeStruct((size, size), F32)
    ring = nf > 1 and size % (SUBLANES * nf) == 0
    if not ring and nf > 1:
        proj = lax.psum(proj, "feat")
    vmem = pl.BlockSpec(memory_space=pltpu.VMEM)
    return pl.pallas_call(
        functools.partial(mix_kernel, subjects, nf, ns, ring),
        out_shape=(square, square, jax.ShapeDtypeStruct(wts.shape, F32), square,
                   jax.ShapeDtypeStruct(proj.shape, F32), square),
        in_specs=[vmem] * 6,
        out_specs=(vmem,) * 6,
        scratch_shapes=ring_scratch(proj.shape, nf, ring)
        + [
            pltpu.VMEM((nf, size, size), F32),
            pltpu.VMEM((ns, size, size), F32),
            pltpu.VMEM((size, size), F32),
            pltpu.VMEM((subjects * size, proj.shape[1]), F32),
            sems(nf), sems(nf), sems(nf), sems(ns),
        ],
        compiler_params=pltpu.CompilerParams(collective_id=0, has_side_effects=True),
        name="mix_step",
    )(proj, vgl, wgram, wts, mix, mask)


def factor_call(ns, total, wgl, hgram):
    size = total.shape[0]
    square = jax.ShapeDtypeStruct((size, size), F32)
    ring = ns > 1 and size % (SUBLANES * ns) == 0
    if not ring and ns > 1:
        total = lax.psum(total, "subj")
    vmem = pl.BlockSpec(memory_space=pltpu.VMEM)
    return pl.pallas_call(
        functools.partial(factor_kernel, ns, ring),
        out_shape=(jax.ShapeDtypeStruct(total.shape, F32), square, square),
        in_specs=[vmem] * 3,
        out_specs=(vmem,) * 3,
        scratch_shapes=ring_scratch(total.shape, ns, ring)
        + [pltpu.VMEM((ns, size, size), F32), sems(ns), sems(ns), sems(ns)],
        compiler_params=pltpu.CompilerParams(collective_id=1, has_side_effects=True),
        name="factor_step",
    )(total, wgl, hgram)


def solution(mesh):
    nf, ns = mesh.shape["feat"], mesh.shape["subj"]

    def per_device(records, feature_factor, mixing, weights, visits):
        subjects = weights.shape[0]
        padded = -(-subjects // SUBLANES) * SUBLANES
        mask = slot_rows(visits, records.shape[0], padded)
        wts = jnp.pad(weights, ((0, padded - subjects), (0, 0)))
        fac = feature_factor.T
        vgl = lax.dot_general(fac, fac, (NT, ((), ())), precision=HIGH, preferred_element_type=F32)
        wgram = lax.psum(
            jnp.dot(weights.T, weights, precision=HIGH, preferred_element_type=F32), "subj"
        )

        def step(_, state):
            fac, vgl, wgram, wts, mix = state
            proj = lax.dot_general(fac, records, (NT, ((), ())), precision=BIG, preferred_element_type=F32)
            mix, hgram, wts, wgl, basis, _ = mix_call(subjects, nf, ns, proj, vgl, wgram, wts, mix, mask)
            total = lax.dot_general(
                basis, records, (((1,), (0,)), ((), ())), precision=BIG, preferred_element_type=F32
            )
            fac, wgram, vgl = factor_call(ns, total, wgl, hgram)
            return fac, vgl, wgram, wts, mix

        fac, _, _, wts, mix = lax.fori_loop(0, ITERS, step, (fac, vgl, wgram, wts, mixing))
        return fac.T, mix, wts[:subjects]

    placed = (P("subj", "feat"), P("feat", None), P(), P("subj", None), P("subj"))
    return jax.shard_map(
        per_device,
        mesh=mesh,
        in_specs=placed,
        out_specs=(P("feat", None), P(), P("subj", None)),
        check_vma=False,
    )
```
